32 devices in a mesh: rows: 8 (over z, y), cols: 4 (over x, core).
Axes of the slice: x: 2, y: 2, z: 4, core: 2. Of those that a mesh axis runs over, the one named last changes fastest.
Arguments:
- panel: float32 [16384, 256], P(('rows', 'cols')), may hold values from -17 to 17, as said below
- trailing: float32 [16384, 2048], P('rows', 'cols'), may hold values from -6 to 6
Outputs:
- rfactor: float32 [256, 256], replicated
- projected: float32 [256, 2048], P(None, 'cols')
- updated: float32 [16384, 2048], P('rows', 'cols')
The draws below stay inside these ranges and needn't reach their ends.
Inputs may be any that keep to these rules, and one draw needn't show every extreme that they name: The panel has full column rank with a moderate condition number (under 100); each column has its own scale and a part shared by all columns.
All inputs are finite; a program needn't handle non-finite values.
Results may differ from the reference program's by a relative error of at most 0.000078.
Values sent between devices are 32-bit elements; how exact they have to be, the bound alone decides.
A program may use at most 64 MiB of HBM per device.

```python
import jax
import jax.numpy as jnp
from jax import lax

PANEL = 256
TRAIL = 2048
ROWS = 16384
PIECE = 512


def draw_panel(key, part):
    keys = jax.random.split(jax.random.fold_in(key, 17), 5)
    noise = jnp.clip(jax.random.normal(keys[0], (ROWS, PANEL), jnp.float32), -6.0, 6.0)
    pieces = ROWS // PIECE
    piece_of_row = jnp.arange(ROWS) // PIECE
    scales = jnp.exp(jax.random.uniform(keys[1], (PANEL,), jnp.float32, jnp.log(0.5), jnp.log(2.0)))
    common = jnp.clip(jax.random.normal(keys[2], (ROWS,), jnp.float32), -5.0, 5.0)
    tilt = jax.random.uniform(keys[3], (PANEL,), jnp.float32, -0.7, 0.7)
    boosted = jax.random.randint(keys[4], (pieces,), 0, PANEL)
    column_ids = jnp.arange(PANEL)
    boost = 1.0 + 5.0 * (column_ids[None, :] == boosted[piece_of_row][:, None]).astype(jnp.float32)
    values = (noise * scales[None, :] + common[:, None] * tilt[None, :]) * boost
    return (values / jnp.sqrt(jnp.float32(ROWS))).astype(jnp.float32)


def levels(stream_key, shape, cuts, smallest, largest):
    level, own = 1.0, jax.random.fold_in(stream_key, 6)
    for axis_at, parts in cuts:
        draws = jnp.exp(jax.random.uniform(jax.random.fold_in(own, axis_at), (parts,), jnp.float32, smallest / len(cuts), largest / len(cuts)))
        level = level * jnp.repeat(draws, shape[axis_at] // parts).reshape([-1 if axis == axis_at else 1 for axis in range(len(shape))])
    return level


def gaussian(stream_key, dims, deviation, bound, cuts=(), held_as=jnp.bfloat16):
    entries = deviation * jax.random.normal(stream_key, dims, jnp.float32)
    if cuts:
        entries = entries * levels(stream_key, dims, cuts, -0.22, 0.18)
    return jnp.clip(entries, -bound, bound).astype(held_as)


def setup_inputs(seed: int = 0) -> dict:
    arg_keys = jax.random.split(jax.random.key(seed), 3)
    return {
        "panel": draw_panel(jax.random.fold_in(arg_keys[2], 71), 0),
        "trailing": gaussian(arg_keys[1], (ROWS, TRAIL), 1.0, 6.0, ((0, 8), (1, 4)), jnp.float32),
    }


def inner(left, right):
    return lax.dot_general(left.astype(jnp.float32), right.astype(jnp.float32), (((0,), (0,)), ((), ())), precision=lax.Precision.HIGHEST, preferred_element_type=jnp.float32)

def reference(panel, trailing):
    gram = inner(panel, panel)
    rfactor = jnp.linalg.cholesky(gram).T
    basis = jax.scipy.linalg.solve_triangular(rfactor.T, panel.T, lower=True).T
    cross = inner(panel, trailing)
    projected = jax.scipy.linalg.solve_triangular(rfactor.T, cross, lower=True)
    updated = trailing - jnp.dot(basis.astype(jnp.float32), projected.astype(jnp.float32), precision=lax.Precision.HIGHEST, preferred_element_type=jnp.float32)
    return (rfactor, projected, updated)
```

```python
import functools

import jax
import jax.numpy as jnp
from jax import lax
from jax.experimental import pallas as pl
from jax.experimental.pallas import tpu as pltpu
from jax.sharding import PartitionSpec as P

MESH = pl.DeviceIdType.MESH
F32 = jnp.float32
LANES = 128
SUBLANES = 8
STRIP = 32


def contract(left, right, dims):
    return lax.dot_general(
        left, right, (dims, ((), ())), precision=lax.Precision.HIGHEST, preferred_element_type=F32
    )


def halves(x):
    high = x.astype(jnp.bfloat16)
    return high, (x - high.astype(F32)).astype(jnp.bfloat16)


def contract3(left, right, dims):
    dot = functools.partial(
        lax.dot_general, dimension_numbers=(dims, ((), ())), preferred_element_type=F32
    )
    (lh, ll), (rh, rl) = left, right
    return dot(lh, rh) + (dot(lh, rl) + dot(ll, rh))


def factor_strip(start, g_ref, r_ref, y_ref):
    n = g_ref.shape[0]
    row = lax.broadcasted_iota(jnp.int32, (STRIP, LANES), 0)
    col = lax.broadcasted_iota(jnp.int32, (STRIP, LANES), 1)
    rows = pl.ds(start, STRIP)
    parts = []
    first = start // LANES * LANES
    for at in range(first, n, LANES):
        parts.append((r_ref, at, g_ref[rows, at : at + LANES]))
    for at in range(0, start + STRIP, LANES):
        parts.append((y_ref, at, jnp.where(col + at == row + start, 1.0, 0.0).astype(F32)))
    if start:
        left = r_ref[0:start, first : first + LANES][:, start - first : start - first + STRIP]
        right = jnp.concatenate([ref[0:start, at : at + LANES] for ref, at, _ in parts], axis=1)
        done = contract(left, right, ((0,), (0,)))
        parts = [
            (ref, at, x - done[:, LANES * i : LANES * (i + 1)]) for i, (ref, at, x) in enumerate(parts)
        ]
    values = [x for _, _, x in parts]
    shift = start - first
    columns = [
        jnp.broadcast_to(values[0][:, shift + i : shift + i + 1], (STRIP, LANES)) for i in range(STRIP)
    ]
    for i in range(STRIP):
        inverse = lax.rsqrt(columns[i][i : i + 1, :])
        scaled = columns[i] * inverse
        for k in range(i + 1, STRIP):
            base = k // SUBLANES * SUBLANES
            low = columns[k][base:] - scaled[base:] * scaled[k : k + 1, :]
            columns[k] = low if base == 0 else jnp.concatenate([columns[k][:base], low], axis=0)
        factor = jnp.where(row > i, scaled, 0.0)
        for v, x in enumerate(values):
            pivot = x[i : i + 1, :] * inverse
            values[v] = jnp.where(row == i, pivot, x - factor * pivot)
    for (ref, at, _), x in zip(parts, values):
        if ref is r_ref:
            x = jnp.where(col + at >= row + start, x, 0.0)
        else:
            x = jnp.where(col + at <= row + start, x, 0.0)
        ref[rows, at : at + LANES] = x


def gather_and_factor(
    nrows, ncols, panel_ref, trailing_ref, r_ref, y_ref, cross_ref, block_ref,
    held, pieces, gram, gram_in, gram_sum, share, share_in, total,
    load_sem, piece_send, piece_recv, gram_sem, share_sem,
):
    r, c = lax.axis_index("rows"), lax.axis_index("cols")
    count = nrows * ncols
    me = r * ncols + c
    depth, n = panel_ref.shape
    width = trailing_ref.shape[1]
    owners = min(count, n // SUBLANES)
    piece = n // owners
    row_owners = min(nrows, n // SUBLANES)
    row_piece = n // row_owners

    load = pltpu.make_async_copy(trailing_ref, held, load_sem)
    load.start()
    pieces[c] = panel_ref[...]

    bits = [1 << b for b in reversed(range(ncols.bit_length() - 1))]
    known = [0]
    index = 0
    sent = []

    def pass_on(offsets, bit):
        nonlocal index
        out = []
        for offset in offsets:
            slot = jnp.bitwise_xor(c, offset) if offset else c
            source = pieces.at[slot] if offset else panel_ref
            copy = pltpu.make_async_remote_copy(
                src_ref=source, dst_ref=pieces.at[slot],
                send_sem=piece_send.at[index], recv_sem=piece_recv.at[index],
                device_id=(r, jnp.bitwise_xor(c, bit)), device_id_type=MESH,
            )
            copy.start()
            sent.append(copy)
            out.append((offset ^ bit, copy))
            index += 1
        return out

    arrivals = {bit: pass_on([0], bit) for bit in bits}

    gram[...] = contract(panel_ref[...], panel_ref[...], ((0,), (0,)))

    def spread(k, action):
        target = lax.rem(me + k, count)
        copy = pltpu.make_async_remote_copy(
            src_ref=gram.at[pl.ds(pl.multiple_of(target * piece, SUBLANES), piece)],
            dst_ref=gram_in.at[me],
            send_sem=gram_sem.at[0], recv_sem=gram_sem.at[1],
            device_id=(lax.div(target, ncols), lax.rem(target, ncols)), device_id_type=MESH,
        )
        if owners == count:
            action(copy)
        else:
            pl.when(target < owners)(lambda: action(copy))

    def each(n_steps, f):
        def step(k, carry):
            f(k)
            return carry
        lax.fori_loop(1, n_steps, step, 0)

    each(count, lambda k: spread(k, lambda copy: copy.start()))

    for at, bit in enumerate(bits):
        for offset, copy in arrivals[bit]:
            copy.wait_recv()
        for later in bits[at + 1 :]:
            arrivals[later] += pass_on([offset for offset, _ in arrivals[bit]], later)

    def own(body):
        if owners == count:
            body()
        else:
            pl.when(me < owners)(body)

    mine = pl.ds(pl.multiple_of(lax.rem(me, owners) * piece, SUBLANES), piece)

    @own
    def _():
        gram_in[me] = gram[mine, :]
        others = gram_in.at[pl.ds(0, count - 1)]
        pltpu.make_async_copy(others, others, gram_sem.at[1]).wait()
        gram_sum[mine, :] = jnp.sum(gram_in[...], axis=0)

        def give(k):
            target = lax.rem(me + k, count)
            pltpu.make_async_remote_copy(
                src_ref=gram_sum.at[mine], dst_ref=gram_sum.at[mine],
                send_sem=gram_sem.at[2], recv_sem=gram_sem.at[3],
                device_id=(lax.div(target, ncols), lax.rem(target, ncols)), device_id_type=MESH,
            ).start()

        each(count, give)

    load.wait()
    tile = 256
    share[...] = jnp.zeros_like(share)

    def multiply(i, carry):
        at = pl.ds(pl.multiple_of(i * tile, tile), tile)
        flat = pieces.reshape(ncols * depth, n)
        share[...] += contract3(halves(flat[at, :]), halves(held[at, :]), ((0,), (0,)))
        return carry

    lax.fori_loop(0, ncols * depth // tile, multiply, 0)

    def row_target(k):
        return lax.rem(r + k, nrows)

    def deal(k):
        target = row_target(k)

        def go():
            pltpu.make_async_remote_copy(
                src_ref=share.at[pl.ds(pl.multiple_of(target * row_piece, SUBLANES), row_piece)],
                dst_ref=share_in.at[r],
                send_sem=share_sem.at[0], recv_sem=share_sem.at[1],
                device_id=(target, c), device_id_type=MESH,
            ).start()

        if row_owners == nrows:
            go()
        else:
            pl.when(target < row_owners)(go)

    each(nrows, deal)
    block_out = pltpu.make_async_copy(pieces, block_ref, load_sem)
    block_out.start()

    def wait_pieces(ref, times, sem):
        if owners == count or times is None:
            pass

    def gram_arrived():
        if owners == count:
            rest = gram_sum.at[pl.ds(0, n - piece)]
            pltpu.make_async_copy(rest, rest, gram_sem.at[3]).wait()
        else:
            @pl.when(me < owners)
            def _():
                rest = gram_sum.at[pl.ds(0, n - piece)]
                pltpu.make_async_copy(rest, rest, gram_sem.at[3]).wait()

            @pl.when(me >= owners)
            def _():
                pltpu.make_async_copy(gram_sum, gram_sum, gram_sem.at[3]).wait()

    gram_arrived()
    strips = list(range(0, n, STRIP))
    half = len(strips) // 2
    for start in strips[:half]:
        factor_strip(start, gram_sum, r_ref, y_ref)

    def row_own(body):
        if row_owners == nrows:
            body()
        else:
            pl.when(r < row_owners)(body)

    my_rows = pl.ds(pl.multiple_of(lax.rem(r, row_owners) * row_piece, SUBLANES), row_piece)

    @row_own
    def _():
        share_in[r] = share[my_rows, :]
        others = share_in.at[pl.ds(0, nrows - 1)]
        pltpu.make_async_copy(others, others, share_sem.at[1]).wait()
        total[my_rows, :] = jnp.sum(share_in[...], axis=0)

        def give(k):
            pltpu.make_async_remote_copy(
                src_ref=total.at[my_rows], dst_ref=total.at[my_rows],
                send_sem=share_sem.at[2], recv_sem=share_sem.at[3],
                device_id=(row_target(k), c), device_id_type=MESH,
            ).start()

        each(nrows, give)

    for start in strips[half:]:
        if start >= LANES:
            r_ref[start : start + STRIP, 0 : start // LANES * LANES] = jnp.zeros(
                (STRIP, start // LANES * LANES), F32
            )
        factor_strip(start, gram_sum, r_ref, y_ref)
    for start in strips:
        edge = -(-(start + STRIP) // LANES) * LANES
        if edge < n:
            y_ref[start : start + STRIP, edge:n] = jnp.zeros((STRIP, n - edge), F32)

    if row_owners == nrows:
        rest = total.at[pl.ds(0, n - row_piece)]
        pltpu.make_async_copy(rest, rest, share_sem.at[3]).wait()
    else:
        @pl.when(r < row_owners)
        def _():
            rest = total.at[pl.ds(0, n - row_piece)]
            pltpu.make_async_copy(rest, rest, share_sem.at[3]).wait()

        @pl.when(r >= row_owners)
        def _():
            pltpu.make_async_copy(total, total, share_sem.at[3]).wait()
    cross_ref[...] = total[...]

    for copy in sent:
        copy.wait_send()
    for bit in bits[1:]:
        pass

    def sent_all(ref, size, sem, index, limit, last):
        if limit == last:
            gone = ref.at[pl.ds(0, (limit - 1) * size)]
            pltpu.make_async_copy(gone, gone, sem).wait()
        else:
            @pl.when(index < limit)
            def _():
                gone = ref.at[pl.ds(0, (limit - 1) * size)]
                pltpu.make_async_copy(gone, gone, sem).wait()

            @pl.when(index >= limit)
            def _():
                gone = ref.at[pl.ds(0, limit * size)]
                pltpu.make_async_copy(gone, gone, sem).wait()

    sent_all(gram, piece, gram_sem.at[0], me, owners, count)
    sent_all(share, row_piece, share_sem.at[0], r, row_owners, nrows)

    def given_all(ref, sem, index, limit, last):
        def body():
            gone = ref.at[pl.ds(0, last - 1)]
            pltpu.make_async_copy(gone, gone, sem).wait()

        if limit == last:
            body()
        else:
            pl.when(index < limit)(body)

    given_all(gram_in, gram_sem.at[2], me, owners, count)
    given_all(share_in, share_sem.at[2], r, row_owners, nrows)
    block_out.wait()


def update(r_ref, y_ref, cross_ref, block_ref, trailing_ref, r_out, projected_ref, updated_ref, high, low):
    @pl.when(pl.program_id(0) == 0)
    def _():
        r_out[...] = r_ref[...]
        projected = contract(y_ref[...], cross_ref[...], ((1,), (0,)))
        projected_ref[...] = projected
        high[...], low[...] = halves(contract(y_ref[...], projected, ((0,), (0,))))

    product = contract3(halves(block_ref[...]), (high[...], low[...]), ((1,), (0,)))
    updated_ref[...] = trailing_ref[...] - product


def solution(mesh):
    nrows, ncols = mesh.shape["rows"], mesh.shape["cols"]

    def shards(panel, trailing):
        depth, n = panel.shape
        height, width = trailing.shape
        count = nrows * ncols
        owners = min(count, n // SUBLANES)
        row_owners = min(nrows, n // SUBLANES)
        vmem = pl.BlockSpec(memory_space=pltpu.VMEM)
        hbm = pl.BlockSpec(memory_space=pl.ANY)
        r, y, cross, block = pl.pallas_call(
            functools.partial(gather_and_factor, nrows, ncols),
            name="gather_and_factor",
            out_shape=(
                jax.ShapeDtypeStruct((n, n), F32),
                jax.ShapeDtypeStruct((n, n), F32),
                jax.ShapeDtypeStruct((n, width), F32),
                jax.ShapeDtypeStruct((ncols, depth, n), F32),
            ),
            in_specs=[vmem, hbm],
            out_specs=(vmem, vmem, vmem, hbm),
            scratch_shapes=[
                pltpu.VMEM((height, width), F32),
                pltpu.VMEM((ncols, depth, n), F32),
                pltpu.VMEM((n, n), F32),
                pltpu.VMEM((count, n // owners, n), F32),
                pltpu.VMEM((n, n), F32),
                pltpu.VMEM((n, width), F32),
                pltpu.VMEM((nrows, n // row_owners, width), F32),
                pltpu.VMEM((n, width), F32),
                pltpu.SemaphoreType.DMA,
                pltpu.SemaphoreType.DMA((ncols - 1,)),
                pltpu.SemaphoreType.DMA((ncols - 1,)),
                pltpu.SemaphoreType.DMA((4,)),
                pltpu.SemaphoreType.DMA((4,)),
            ],
            compiler_params=pltpu.CompilerParams(has_side_effects=True, vmem_limit_bytes=40 << 20),
        )(panel, trailing)
        block = block.reshape(height, n)
        tile = min(height, 512)
        whole = lambda *shape: pl.BlockSpec(shape, lambda i: (0, 0))
        tall = lambda wide: pl.BlockSpec((tile, wide), lambda i: (i, 0))
        return pl.pallas_call(
            update,
            name="update",
            grid=(height // tile,),
            out_shape=(
                jax.ShapeDtypeStruct((n, n), F32),
                jax.ShapeDtypeStruct((n, width), F32),
                jax.ShapeDtypeStruct((height, width), F32),
            ),
            in_specs=[whole(n, n), whole(n, n), whole(n, width), tall(n), tall(width)],
            out_specs=(whole(n, n), whole(n, width), tall(width)),
            scratch_shapes=[pltpu.VMEM((n, width), jnp.bfloat16)] * 2,
            compiler_params=pltpu.CompilerParams(vmem_limit_bytes=32 << 20),
        )(r, y, cross, block, trailing)

    placed = (P(("rows", "cols"), None), P("rows", "cols"))
    return jax.shard_map(
        shards,
        mesh=mesh,
        in_specs=placed,
        out_specs=(P(), P(None, "cols"), P("rows", "cols")),
        check_vma=False,
    )
```

```python
import functools

import jax
import jax.numpy as jnp
from jax import lax
from jax.experimental import pallas as pl
from jax.experimental.pallas import tpu as pltpu
from jax.sharding import PartitionSpec as P

MESH = pl.DeviceIdType.MESH
F32 = jnp.float32
LANES = 128
SUBLANES = 8
STRIP = 32
CHUNK = 128


def contract(left, right, dims):
    return lax.dot_general(
        left, right, (dims, ((), ())), precision=lax.Precision.HIGHEST, preferred_element_type=F32
    )


def halves(x):
    high = x.astype(jnp.bfloat16)
    return high, (x - high.astype(F32)).astype(jnp.bfloat16)


def contract3(left, right, dims):
    dot = functools.partial(
        lax.dot_general, dimension_numbers=(dims, ((), ())), preferred_element_type=F32
    )
    (lh, ll), (rh, rl) = left, right
    return dot(lh, rh) + (dot(lh, rl) + dot(ll, rh))


def factor_strip(start, g_ref, r_ref, y_ref):
    n = g_ref.shape[0]
    row = lax.broadcasted_iota(jnp.int32, (STRIP, LANES), 0)
    col = lax.broadcasted_iota(jnp.int32, (STRIP, LANES), 1)
    rows = pl.ds(start, STRIP)
    parts = []
    first = start // LANES * LANES
    for at in range(first, n, LANES):
        parts.append((r_ref, at, g_ref[rows, at : at + LANES]))
    for at in range(0, start + STRIP, LANES):
        parts.append((y_ref, at, jnp.where(col + at == row + start, 1.0, 0.0).astype(F32)))
    if start:
        left = r_ref[0:start, first : first + LANES][:, start - first : start - first + STRIP]
        right = jnp.concatenate([ref[0:start, at : at + LANES] for ref, at, _ in parts], axis=1)
        done = contract(left, right, ((0,), (0,)))
        parts = [
            (ref, at, x - done[:, LANES * i : LANES * (i + 1)]) for i, (ref, at, x) in enumerate(parts)
        ]
    values = [x for _, _, x in parts]
    shift = start - first
    columns = [
        jnp.broadcast_to(values[0][:, shift + i : shift + i + 1], (STRIP, LANES)) for i in range(STRIP)
    ]
    for i in range(STRIP):
        inverse = lax.rsqrt(columns[i][i : i + 1, :])
        scaled = columns[i] * inverse
        for k in range(i + 1, STRIP):
            base = k // SUBLANES * SUBLANES
            low = columns[k][base:] - scaled[base:] * scaled[k : k + 1, :]
            columns[k] = low if base == 0 else jnp.concatenate([columns[k][:base], low], axis=0)
        factor = jnp.where(row > i, scaled, 0.0)
        for v, x in enumerate(values):
            pivot = x[i : i + 1, :] * inverse
            values[v] = jnp.where(row == i, pivot, x - factor * pivot)
    for (ref, at, _), x in zip(parts, values):
        if ref is r_ref:
            x = jnp.where(col + at >= row + start, x, 0.0)
        else:
            x = jnp.where(col + at <= row + start, x, 0.0)
        ref[rows, at : at + LANES] = x


class Direct:
    def __init__(self, members, member, device, size, source, landing, result, base, sems):
        self.members, self.member, self.device = members, member, device
        self.source, self.landing, self.result, self.base, self.sems = source, landing, result, base, sems
        self.owners = min(members, size // SUBLANES)
        self.piece = size // self.owners

    def rows(self, index, base=0):
        return pl.ds(pl.multiple_of(base + index * self.piece, SUBLANES), self.piece)

    def if_owner(self, index, body):
        if self.owners == self.members:
            body()
        else:
            pl.when(index < self.owners)(body)

    def each(self, body):
        def step(k, carry):
            body(lax.rem(self.member + k, self.members))
            return carry

        lax.fori_loop(1, self.members, step, 0, unroll=self.members <= 4)

    def wait(self, ref, sem):
        pltpu.make_async_copy(ref, ref, sem).wait()

    def wait_parts(self, sem):
        def whole(parts):
            self.wait(self.result.at[pl.ds(0, parts * self.piece)], sem)

        if self.owners == self.members:
            whole(self.owners - 1)
        else:
            pl.when(self.member < self.owners)(lambda: whole(self.owners - 1))
            pl.when(self.member >= self.owners)(lambda: whole(self.owners))

    def scatter(self):
        def send(target):
            self.if_owner(target, lambda: pltpu.make_async_remote_copy(
                src_ref=self.source.at[self.rows(target)], dst_ref=self.landing.at[self.member],
                send_sem=self.sems.at[0], recv_sem=self.sems.at[1],
                device_id=self.device(target), device_id_type=MESH,
            ).start())

        self.each(send)

    def reduce(self):
        @functools.partial(self.if_owner, self.member)
        def _():
            index = lax.rem(self.member, self.owners)
            mine = self.rows(index, self.base)
            self.landing[self.member] = self.source[self.rows(index), :]
            self.wait(self.landing.at[pl.ds(0, self.members - 1)], self.sems.at[1])
            self.result[mine, :] = jnp.sum(self.landing[...], axis=0)
            self.each(lambda target: pltpu.make_async_remote_copy(
                src_ref=self.result.at[mine], dst_ref=self.result.at[mine],
                send_sem=self.sems.at[2], recv_sem=self.sems.at[3],
                device_id=self.device(target), device_id_type=MESH,
            ).start())

    def arrived(self):
        self.wait_parts(self.sems.at[3])

    def finish(self):
        self.wait_parts(self.sems.at[0])
        self.if_owner(self.member, lambda: self.wait(
            self.landing.at[pl.ds(0, self.members - 1)], self.sems.at[2]))


class Pair:
    def __init__(self, side, device, half, source, base, landing, kept, sems):
        self.device, self.source, self.landing, self.kept, self.sems = device, source, landing, kept, sems
        self.mine = pl.ds(pl.multiple_of(base + side * half, SUBLANES), half)
        self.other = pl.ds(pl.multiple_of(base + (1 - side) * half, SUBLANES), half)

    def scatter(self):
        self.out = pltpu.make_async_remote_copy(
            src_ref=self.source.at[self.other], dst_ref=self.landing,
            send_sem=self.sems.at[0], recv_sem=self.sems.at[1],
            device_id=self.device, device_id_type=MESH,
        )
        self.out.start()

    def reduce(self):
        self.out.wait_recv()
        self.kept[...] = self.source[self.mine, :] + self.landing[...]

    def gather(self, result):
        self.back = pltpu.make_async_remote_copy(
            src_ref=result.at[self.mine], dst_ref=result.at[self.mine],
            send_sem=self.sems.at[2], recv_sem=self.sems.at[3],
            device_id=self.device, device_id_type=MESH,
        )
        self.back.start()

    def arrived(self):
        self.back.wait_recv()

    def finish(self):
        self.out.wait_send()
        self.back.wait_send()


def gather_and_factor(
    nrows, ncols, panel_ref, trailing_ref, r_ref, y_ref, cross_ref, block_ref,
    held, high, low, pieces, gram, gram_near, gram_pair, gram_in, gram_sum,
    share, share_near, share_pair, share_in, total,
    load_sem, piece_send, piece_recv, gram_pair_sem, gram_sem, share_pair_sem, share_sem,
):
    r, c = lax.axis_index("rows"), lax.axis_index("cols")
    depth, n = panel_ref.shape
    chunks = n // CHUNK

    own_load = pltpu.make_async_copy(panel_ref, pieces.at[c], load_sem.at[0])
    own_load.start()
    load = pltpu.make_async_copy(trailing_ref, held, load_sem.at[1])
    load.start()
    own_load.wait()

    bits = [1 << b for b in reversed(range(ncols.bit_length() - 1))]
    sent = []

    def pass_on(offset, bit, chunk):
        slot = jnp.bitwise_xor(c, offset)
        view = pieces.at[slot, :, pl.ds(chunk * CHUNK, CHUNK)]
        copy = pltpu.make_async_remote_copy(
            src_ref=view, dst_ref=view,
            send_sem=piece_send.at[len(sent)], recv_sem=piece_recv.at[len(sent)],
            device_id=(r, jnp.bitwise_xor(c, bit)), device_id_type=MESH,
        )
        copy.start()
        sent.append(copy)
        return offset ^ bit, copy

    coming = {(bit, chunk): [pass_on(0, bit, chunk)] for chunk in range(chunks) for bit in bits}

    gram[...] = contract(pieces[c], pieces[c], ((0,), (0,)))
    side, wide = lax.rem(c, 2), ncols // 2
    gram_halves = Pair(side, (r, jnp.bitwise_xor(c, 1)), n // 2, gram, 0, gram_near, gram_pair, gram_pair_sem)
    gram_halves.scatter()
    gram_all = Direct(
        nrows * wide, r * wide + lax.div(c, 2),
        lambda t: (lax.div(t, wide), lax.rem(t, wide) * 2 + side),
        n // 2, gram_pair, gram_in, gram_sum, side * (n // 2), gram_sem,
    )
    upper = lax.rem(r, 2)
    pairs, groups = [], []
    for h in range(chunks):
        half = CHUNK // 2
        pairs.append(Pair(
            upper, (jnp.bitwise_xor(r, 1), c), half, share, h * CHUNK,
            share_near.at[h], share_pair.at[h], share_pair_sem.at[h],
        ))
        groups.append(Direct(
            nrows // 2, lax.div(r, 2), lambda t: (t * 2 + upper, c),
            half, share_pair.at[h], share_in.at[h], total, h * CHUNK + upper * half, share_sem.at[h],
        ))

    load.wait()

    def split(i, carry):
        at = pl.ds(pl.multiple_of(i * LANES, LANES), LANES)
        high[at, :], low[at, :] = halves(held[at, :])
        return carry

    lax.fori_loop(0, held.shape[0] // LANES, split, 0)
    gram_halves.reduce()
    gram_all.scatter()

    def multiply(offset, h, first=False):
        slot = jnp.bitwise_xor(c, offset)
        at = pl.ds(pl.multiple_of(slot * depth, LANES), depth)
        mine = slice(h * CHUNK, (h + 1) * CHUNK)
        product = contract3(halves(pieces[slot, :, mine]), (high[at, :], low[at, :]), ((0,), (0,)))
        share[mine, :] = product if first else share[mine, :] + product

    for h in range(chunks):
        multiply(0, h, True)
    for h in range(chunks):
        offset, copy = coming[bits[-1], h].pop(0)
        copy.wait_recv()
        multiply(offset, h)

    def take(h):
        for at, bit in enumerate(bits):
            for offset, copy in coming[bit, h]:
                copy.wait_recv()
                for later in bits[at + 1 :]:
                    coming[later, h].append(pass_on(offset, later, h))
                multiply(offset, h)
        pairs[h].scatter()

    strips = list(range(0, n, STRIP))

    def factor(some):
        for start in some:
            if start >= LANES:
                r_ref[start : start + STRIP, 0 : start // LANES * LANES] = jnp.zeros(
                    (STRIP, start // LANES * LANES), F32
                )
            edge = -(-(start + STRIP) // LANES) * LANES
            if edge < n:
                y_ref[start : start + STRIP, edge:n] = jnp.zeros((STRIP, n - edge), F32)
            factor_strip(start, gram_sum, r_ref, y_ref)

    take(0)
    gram_all.reduce()
    for h in range(1, chunks):
        pairs[h - 1].reduce()
        groups[h - 1].scatter()
        take(h)
        groups[h - 1].reduce()
    block_out = pltpu.make_async_copy(pieces, block_ref, load_sem.at[1])
    block_out.start()
    gram_all.arrived()
    gram_halves.gather(gram_sum)
    pairs[-1].reduce()
    groups[-1].scatter()
    gram_halves.arrived()
    half = len(strips) // 2
    factor(strips[:half])
    groups[-1].reduce()
    for h in range(chunks - 1):
        groups[h].arrived()
        pairs[h].gather(total)
    factor(strips[half:])
    groups[-1].arrived()
    pairs[-1].gather(total)
    for pair in pairs:
        pair.arrived()
    cross_ref[...] = total[...]
    for copy in sent:
        copy.wait_send()
    for exchange in [gram_halves, gram_all] + pairs + groups:
        exchange.finish()
    block_out.wait()


def update(r_ref, y_ref, cross_ref, block_ref, trailing_ref, r_out, projected_ref, updated_ref, high, low):
    @pl.when(pl.program_id(0) == 0)
    def _():
        r_out[...] = r_ref[...]
        projected = contract(y_ref[...], cross_ref[...], ((1,), (0,)))
        projected_ref[...] = projected
        high[...], low[...] = halves(contract(y_ref[...], projected, ((0,), (0,))))

    product = contract3(halves(block_ref[...]), (high[...], low[...]), ((1,), (0,)))
    updated_ref[...] = trailing_ref[...] - product


def solution(mesh):
    nrows, ncols = mesh.shape["rows"], mesh.shape["cols"]

    def shards(panel, trailing):
        depth, n = panel.shape
        height, width = trailing.shape
        chunks = n // CHUNK
        half = CHUNK // 2
        group = nrows * ncols // 2
        vmem = pl.BlockSpec(memory_space=pltpu.VMEM)
        hbm = pl.BlockSpec(memory_space=pl.ANY)
        r, y, cross, block = pl.pallas_call(
            functools.partial(gather_and_factor, nrows, ncols),
            name="gather_and_factor",
            out_shape=(
                jax.ShapeDtypeStruct((n, n), F32),
                jax.ShapeDtypeStruct((n, n), F32),
                jax.ShapeDtypeStruct((n, width), F32),
                jax.ShapeDtypeStruct((ncols, depth, n), F32),
            ),
            in_specs=[hbm, hbm],
            out_specs=(vmem, vmem, vmem, hbm),
            scratch_shapes=[
                pltpu.VMEM((height, width), F32),
                pltpu.VMEM((height, width), jnp.bfloat16),
                pltpu.VMEM((height, width), jnp.bfloat16),
                pltpu.VMEM((ncols, depth, n), F32),
                pltpu.VMEM((n, n), F32),
                pltpu.VMEM((n // 2, n), F32),
                pltpu.VMEM((n // 2, n), F32),
                pltpu.VMEM((group, n // 2 // min(group, n // 2 // SUBLANES), n), F32),
                pltpu.VMEM((n, n), F32),
                pltpu.VMEM((n, width), F32),
                pltpu.VMEM((chunks, half, width), F32),
                pltpu.VMEM((chunks, half, width), F32),
                pltpu.VMEM((chunks, nrows // 2, half // min(nrows // 2, half // SUBLANES), width), F32),
                pltpu.VMEM((n, width), F32),
                pltpu.SemaphoreType.DMA((2,)),
                pltpu.SemaphoreType.DMA(((ncols - 1) * chunks,)),
                pltpu.SemaphoreType.DMA(((ncols - 1) * chunks,)),
                pltpu.SemaphoreType.DMA((4,)),
                pltpu.SemaphoreType.DMA((4,)),
                pltpu.SemaphoreType.DMA((chunks, 4)),
                pltpu.SemaphoreType.DMA((chunks, 4)),
            ],
            compiler_params=pltpu.CompilerParams(has_side_effects=True, vmem_limit_bytes=67043328),
        )(panel, trailing)
        block = block.reshape(height, n)
        tile = min(height, 512)
        whole = lambda *shape: pl.BlockSpec(shape, lambda i: (0, 0))
        tall = lambda wide: pl.BlockSpec((tile, wide), lambda i: (i, 0))
        return pl.pallas_call(
            update,
            name="update",
            grid=(height // tile,),
            out_shape=(
                jax.ShapeDtypeStruct((n, n), F32),
                jax.ShapeDtypeStruct((n, width), F32),
                jax.ShapeDtypeStruct((height, width), F32),
            ),
            in_specs=[whole(n, n), whole(n, n), whole(n, width), tall(n), tall(width)],
            out_specs=(whole(n, n), whole(n, width), tall(width)),
            scratch_shapes=[pltpu.VMEM((n, width), jnp.bfloat16)] * 2,
            compiler_params=pltpu.CompilerParams(vmem_limit_bytes=32 << 20),
        )(r, y, cross, block, trailing)

    placed = (P(("rows", "cols"), None), P("rows", "cols"))
    return jax.shard_map(
        shards,
        mesh=mesh,
        in_specs=placed,
        out_specs=(P(), P(None, "cols"), P("rows", "cols")),
        check_vma=False,
    )
```

```python
import functools

import jax
import jax.numpy as jnp
from jax import lax
from jax.experimental import pallas as pl
from jax.experimental.pallas import tpu as pltpu
from jax.sharding import PartitionSpec as P

MESH = pl.DeviceIdType.MESH
F32 = jnp.float32
LANES = 128
SUBLANES = 8
STRIP = 32
CHUNK = 128


def contract(left, right, dims):
    return lax.dot_general(
        left, right, (dims, ((), ())), precision=lax.Precision.HIGHEST, preferred_element_type=F32
    )


def halves(x):
    high = x.astype(jnp.bfloat16)
    return high, (x - high.astype(F32)).astype(jnp.bfloat16)


def contract3(left, right, dims):
    dot = functools.partial(
        lax.dot_general, dimension_numbers=(dims, ((), ())), preferred_element_type=F32
    )
    (lh, ll), (rh, rl) = left, right
    return dot(lh, rh) + (dot(lh, rl) + dot(ll, rh))


def factor_strip(start, g_ref, r_ref, y_ref):
    n = g_ref.shape[0]
    row = lax.broadcasted_iota(jnp.int32, (STRIP, LANES), 0)
    col = lax.broadcasted_iota(jnp.int32, (STRIP, LANES), 1)
    rows = pl.ds(start, STRIP)
    parts = []
    first = start // LANES * LANES
    for at in range(first, n, LANES):
        parts.append((r_ref, at, g_ref[rows, at : at + LANES]))
    for at in range(0, start + STRIP, LANES):
        parts.append((y_ref, at, jnp.where(col + at == row + start, 1.0, 0.0).astype(F32)))
    if start:
        left = r_ref[0:start, first : first + LANES][:, start - first : start - first + STRIP]
        right = jnp.concatenate([ref[0:start, at : at + LANES] for ref, at, _ in parts], axis=1)
        done = contract(left, right, ((0,), (0,)))
        parts = [
            (ref, at, x - done[:, LANES * i : LANES * (i + 1)]) for i, (ref, at, x) in enumerate(parts)
        ]
    values = [x for _, _, x in parts]
    shift = start - first
    columns = [
        jnp.broadcast_to(values[0][:, shift + i : shift + i + 1], (STRIP, LANES)) for i in range(STRIP)
    ]
    for i in range(STRIP):
        inverse = lax.rsqrt(columns[i][i : i + 1, :])
        scaled = columns[i] * inverse
        for k in range(i + 1, STRIP):
            base = k // SUBLANES * SUBLANES
            low = columns[k][base:] - scaled[base:] * scaled[k : k + 1, :]
            columns[k] = low if base == 0 else jnp.concatenate([columns[k][:base], low], axis=0)
        factor = jnp.where(row > i, scaled, 0.0)
        for v, x in enumerate(values):
            pivot = x[i : i + 1, :] * inverse
            values[v] = jnp.where(row == i, pivot, x - factor * pivot)
    for (ref, at, _), x in zip(parts, values):
        if ref is r_ref:
            x = jnp.where(col + at >= row + start, x, 0.0)
        else:
            x = jnp.where(col + at <= row + start, x, 0.0)
        ref[rows, at : at + LANES] = x


class Direct:
    def __init__(self, members, member, device, size, source, landing, result, base, sems):
        self.members, self.member, self.device = members, member, device
        self.source, self.landing, self.result, self.base, self.sems = source, landing, result, base, sems
        self.owners = min(members, size // SUBLANES)
        self.piece = size // self.owners

    def rows(self, index, base=0):
        return pl.ds(pl.multiple_of(base + index * self.piece, SUBLANES), self.piece)

    def if_owner(self, index, body):
        if self.owners == self.members:
            body()
        else:
            pl.when(index < self.owners)(body)

    def each(self, body):
        def step(k, carry):
            body(lax.rem(self.member + k, self.members))
            return carry

        lax.fori_loop(1, self.members, step, 0, unroll=self.members <= 4)

    def wait(self, ref, sem):
        pltpu.make_async_copy(ref, ref, sem).wait()

    def wait_parts(self, sem):
        def whole(parts):
            self.wait(self.result.at[pl.ds(0, parts * self.piece)], sem)

        if self.owners == self.members:
            whole(self.owners - 1)
        else:
            pl.when(self.member < self.owners)(lambda: whole(self.owners - 1))
            pl.when(self.member >= self.owners)(lambda: whole(self.owners))

    def scatter(self):
        def send(target):
            self.if_owner(target, lambda: pltpu.make_async_remote_copy(
                src_ref=self.source.at[self.rows(target)], dst_ref=self.landing.at[self.member],
                send_sem=self.sems.at[0], recv_sem=self.sems.at[1],
                device_id=self.device(target), device_id_type=MESH,
            ).start())

        self.each(send)

    def reduce(self):
        @functools.partial(self.if_owner, self.member)
        def _():
            index = lax.rem(self.member, self.owners)
            mine = self.rows(index, self.base)
            self.landing[self.member] = self.source[self.rows(index), :]
            self.wait(self.landing.at[pl.ds(0, self.members - 1)], self.sems.at[1])
            self.result[mine, :] = jnp.sum(self.landing[...], axis=0)
            self.each(lambda target: pltpu.make_async_remote_copy(
                src_ref=self.result.at[mine], dst_ref=self.result.at[mine],
                send_sem=self.sems.at[2], recv_sem=self.sems.at[3],
                device_id=self.device(target), device_id_type=MESH,
            ).start())

    def arrived(self):
        self.wait_parts(self.sems.at[3])

    def finish(self):
        self.wait_parts(self.sems.at[0])
        self.if_owner(self.member, lambda: self.wait(
            self.landing.at[pl.ds(0, self.members - 1)], self.sems.at[2]))


class Pair:
    def __init__(self, side, device, half, source, base, landing, kept, sems):
        self.device, self.source, self.landing, self.kept, self.sems = device, source, landing, kept, sems
        self.mine = pl.ds(pl.multiple_of(base + side * half, SUBLANES), half)
        self.other = pl.ds(pl.multiple_of(base + (1 - side) * half, SUBLANES), half)

    def scatter(self):
        self.out = pltpu.make_async_remote_copy(
            src_ref=self.source.at[self.other], dst_ref=self.landing,
            send_sem=self.sems.at[0], recv_sem=self.sems.at[1],
            device_id=self.device, device_id_type=MESH,
        )
        self.out.start()

    def reduce(self):
        self.out.wait_recv()
        self.kept[...] = self.source[self.mine, :] + self.landing[...]

    def gather(self, result):
        self.back = pltpu.make_async_remote_copy(
            src_ref=result.at[self.mine], dst_ref=result.at[self.mine],
            send_sem=self.sems.at[2], recv_sem=self.sems.at[3],
            device_id=self.device, device_id_type=MESH,
        )
        self.back.start()

    def arrived(self):
        self.back.wait_recv()

    def finish(self):
        self.out.wait_send()
        self.back.wait_send()


def gather_and_factor(
    nrows, ncols, panel_ref, trailing_ref, r_ref, y_ref, cross_ref, block_ref,
    held, high, low, pieces, gram, gram_near, gram_pair, gram_in, gram_sum,
    share, share_near, share_pair, share_in, total,
    load_sem, piece_send, piece_recv, gram_pair_sem, gram_sem, share_pair_sem, share_sem,
):
    r, c = lax.axis_index("rows"), lax.axis_index("cols")
    depth, n = panel_ref.shape
    chunks = n // CHUNK

    own_load = pltpu.make_async_copy(panel_ref, pieces.at[c], load_sem.at[0])
    own_load.start()
    load = pltpu.make_async_copy(trailing_ref, held, load_sem.at[1])
    load.start()
    own_load.wait()

    bits = [1 << b for b in reversed(range(ncols.bit_length() - 1))]
    sent = []

    def pass_on(offset, bit, chunk):
        slot = jnp.bitwise_xor(c, offset)
        view = pieces.at[slot, :, pl.ds(chunk * CHUNK, CHUNK)]
        copy = pltpu.make_async_remote_copy(
            src_ref=view, dst_ref=view,
            send_sem=piece_send.at[len(sent)], recv_sem=piece_recv.at[len(sent)],
            device_id=(r, jnp.bitwise_xor(c, bit)), device_id_type=MESH,
        )
        copy.start()
        sent.append(copy)
        return offset ^ bit, copy

    coming = {(bit, chunk): [pass_on(0, bit, chunk)] for chunk in range(chunks) for bit in bits}

    gram[...] = contract(pieces[c], pieces[c], ((0,), (0,)))
    side, wide = lax.rem(c, 2), ncols // 2
    gram_halves = Pair(side, (r, jnp.bitwise_xor(c, 1)), n // 2, gram, 0, gram_near, gram_pair, gram_pair_sem)
    gram_halves.scatter()
    gram_all = Direct(
        nrows * wide, r * wide + lax.div(c, 2),
        lambda t: (lax.div(t, wide), lax.rem(t, wide) * 2 + side),
        n // 2, gram_pair, gram_in, gram_sum, side * (n // 2), gram_sem,
    )
    upper = lax.rem(r, 2)
    pairs, groups = [], []
    for h in range(chunks):
        half = CHUNK // 2
        pairs.append(Pair(
            upper, (jnp.bitwise_xor(r, 1), c), half, share, h * CHUNK,
            share_near.at[h], share_pair.at[h], share_pair_sem.at[h],
        ))
        groups.append(Direct(
            nrows // 2, lax.div(r, 2), lambda t: (t * 2 + upper, c),
            half, share_pair.at[h], share_in.at[h], total, h * CHUNK + upper * half, share_sem.at[h],
        ))

    load.wait()

    def split(i, carry):
        at = pl.ds(pl.multiple_of(i * LANES, LANES), LANES)
        high[at, :], low[at, :] = halves(held[at, :])
        return carry

    lax.fori_loop(0, held.shape[0] // LANES, split, 0)
    gram_halves.reduce()
    gram_all.scatter()

    def multiply(offset, h, first=False):
        slot = jnp.bitwise_xor(c, offset)
        at = pl.ds(pl.multiple_of(slot * depth, LANES), depth)
        mine = slice(h * CHUNK, (h + 1) * CHUNK)
        product = contract3(halves(pieces[slot, :, mine]), (high[at, :], low[at, :]), ((0,), (0,)))
        share[mine, :] = product if first else share[mine, :] + product

    for h in range(chunks):
        multiply(0, h, True)
    for h in range(chunks):
        offset, copy = coming[bits[-1], h].pop(0)
        copy.wait_recv()
        multiply(offset, h)

    def take(h):
        for at, bit in enumerate(bits):
            for offset, copy in coming[bit, h]:
                copy.wait_recv()
                for later in bits[at + 1 :]:
                    coming[later, h].append(pass_on(offset, later, h))
                multiply(offset, h)
        pairs[h].scatter()

    strips = list(range(0, n, STRIP))

    def factor(some):
        for start in some:
            if start >= LANES:
                r_ref[start : start + STRIP, 0 : start // LANES * LANES] = jnp.zeros(
                    (STRIP, start // LANES * LANES), F32
                )
            edge = -(-(start + STRIP) // LANES) * LANES
            if edge < n:
                y_ref[start : start + STRIP, edge:n] = jnp.zeros((STRIP, n - edge), F32)
            factor_strip(start, gram_sum, r_ref, y_ref)

    take(0)
    gram_all.reduce()
    for h in range(1, chunks):
        pairs[h - 1].reduce()
        groups[h - 1].scatter()
        take(h)
        groups[h - 1].reduce()
    block_out = pltpu.make_async_copy(pieces, block_ref, load_sem.at[1])
    block_out.start()
    gram_all.arrived()
    gram_halves.gather(gram_sum)
    pairs[-1].reduce()
    groups[-1].scatter()
    gram_halves.arrived()
    half = len(strips) // 2
    factor(strips[:half])
    groups[-1].reduce()
    for h in range(chunks - 1):
        groups[h].arrived()
        pairs[h].gather(total)
    factor(strips[half:])
    groups[-1].arrived()
    pairs[-1].gather(total)
    for pair in pairs:
        pair.arrived()
    cross_ref[...] = total[...]
    for copy in sent:
        copy.wait_send()
    for exchange in [gram_halves, gram_all] + pairs + groups:
        exchange.finish()
    block_out.wait()


def update(r_ref, y_ref, cross_ref, block_ref, trailing_ref, r_out, projected_ref, updated_ref, high, low):
    @pl.when(pl.program_id(0) == 0)
    def _():
        r_out[...] = r_ref[...]
        projected = contract(y_ref[...], cross_ref[...], ((1,), (0,)))
        projected_ref[...] = projected
        high[...], low[...] = halves(contract(y_ref[...], projected, ((0,), (0,))))

    product = contract3(halves(block_ref[...]), (high[...], low[...]), ((1,), (0,)))
    updated_ref[...] = trailing_ref[...] - product


def solution(mesh):
    nrows, ncols = mesh.shape["rows"], mesh.shape["cols"]

    def shards(panel, trailing):
        depth, n = panel.shape
        height, width = trailing.shape
        chunks = n // CHUNK
        half = CHUNK // 2
        group = nrows * ncols // 2
        vmem = pl.BlockSpec(memory_space=pltpu.VMEM)
        hbm = pl.BlockSpec(memory_space=pl.ANY)
        r, y, cross, block = pl.pallas_call(
            functools.partial(gather_and_factor, nrows, ncols),
            name="gather_and_factor",
            out_shape=(
                jax.ShapeDtypeStruct((n, n), F32),
                jax.ShapeDtypeStruct((n, n), F32),
                jax.ShapeDtypeStruct((n, width), F32),
                jax.ShapeDtypeStruct((ncols, depth, n), F32),
            ),
            in_specs=[hbm, hbm],
            out_specs=(vmem, vmem, vmem, hbm),
            scratch_shapes=[
                pltpu.VMEM((height, width), F32),
                pltpu.VMEM((height, width), jnp.bfloat16),
                pltpu.VMEM((height, width), jnp.bfloat16),
                pltpu.VMEM((ncols, depth, n), F32),
                pltpu.VMEM((n, n), F32),
                pltpu.VMEM((n // 2, n), F32),
                pltpu.VMEM((n // 2, n), F32),
                pltpu.VMEM((group, n // 2 // min(group, n // 2 // SUBLANES), n), F32),
                pltpu.VMEM((n, n), F32),
                pltpu.VMEM((n, width), F32),
                pltpu.VMEM((chunks, half, width), F32),
                pltpu.VMEM((chunks, half, width), F32),
                pltpu.VMEM((chunks, nrows // 2, half // min(nrows // 2, half // SUBLANES), width), F32),
                pltpu.VMEM((n, width), F32),
                pltpu.SemaphoreType.DMA((2,)),
                pltpu.SemaphoreType.DMA(((ncols - 1) * chunks,)),
                pltpu.SemaphoreType.DMA(((ncols - 1) * chunks,)),
                pltpu.SemaphoreType.DMA((4,)),
                pltpu.SemaphoreType.DMA((4,)),
                pltpu.SemaphoreType.DMA((chunks, 4)),
                pltpu.SemaphoreType.DMA((chunks, 4)),
            ],
            compiler_params=pltpu.CompilerParams(has_side_effects=True, vmem_limit_bytes=67043328),
        )(panel, trailing)
        block = block.reshape(height, n)
        tile = min(height, 512)
        whole = lambda *shape: pl.BlockSpec(shape, lambda i: (0, 0))
        tall = lambda wide: pl.BlockSpec((tile, wide), lambda i: (i, 0))
        return pl.pallas_call(
            update,
            name="update",
            grid=(height // tile,),
            out_shape=(
                jax.ShapeDtypeStruct((n, n), F32),
                jax.ShapeDtypeStruct((n, width), F32),
                jax.ShapeDtypeStruct((height, width), F32),
            ),
            in_specs=[whole(n, n), whole(n, n), whole(n, width), tall(n), tall(width)],
            out_specs=(whole(n, n), whole(n, width), tall(width)),
            scratch_shapes=[pltpu.VMEM((n, width), jnp.bfloat16)] * 2,
            compiler_params=pltpu.CompilerParams(vmem_limit_bytes=67043328),
        )(r, y, cross, block, trailing)

    placed = (P(("rows", "cols"), None), P("rows", "cols"))
    return jax.shard_map(
        shards,
        mesh=mesh,
        in_specs=placed,
        out_specs=(P(), P(None, "cols"), P("rows", "cols")),
        check_vma=False,
    )
```

```python
import functools

import jax
import jax.numpy as jnp
from jax import lax
from jax.experimental import pallas as pl
from jax.experimental.pallas import tpu as pltpu
from jax.sharding import PartitionSpec as P

MESH = pl.DeviceIdType.MESH
F32 = jnp.float32
LANES = 128
SUBLANES = 8
STRIP = 32
CHUNK = 128


def contract(left, right, dims):
    return lax.dot_general(
        left, right, (dims, ((), ())), precision=lax.Precision.HIGHEST, preferred_element_type=F32
    )


def halves(x):
    high = x.astype(jnp.bfloat16)
    return high, (x - high.astype(F32)).astype(jnp.bfloat16)


def contract3(left, right, dims):
    dot = functools.partial(
        lax.dot_general, dimension_numbers=(dims, ((), ())), preferred_element_type=F32
    )
    (lh, ll), (rh, rl) = left, right
    return dot(lh, rh) + (dot(lh, rl) + dot(ll, rh))


def factor_strip(start, g_ref, r_ref, y_ref):
    n = g_ref.shape[0]
    row = lax.broadcasted_iota(jnp.int32, (STRIP, LANES), 0)
    col = lax.broadcasted_iota(jnp.int32, (STRIP, LANES), 1)
    rows = pl.ds(start, STRIP)
    parts = []
    first = start // LANES * LANES
    for at in range(first, n, LANES):
        parts.append((r_ref, at, g_ref[rows, at : at + LANES]))
    for at in range(0, start + STRIP, LANES):
        parts.append((y_ref, at, jnp.where(col + at == row + start, 1.0, 0.0).astype(F32)))
    if start:
        left = r_ref[0:start, first : first + LANES][:, start - first : start - first + STRIP]
        right = jnp.concatenate([ref[0:start, at : at + LANES] for ref, at, _ in parts], axis=1)
        done = contract(left, right, ((0,), (0,)))
        parts = [
            (ref, at, x - done[:, LANES * i : LANES * (i + 1)]) for i, (ref, at, x) in enumerate(parts)
        ]
    values = [x for _, _, x in parts]
    shift = start - first
    columns = [
        jnp.broadcast_to(values[0][:, shift + i : shift + i + 1], (STRIP, LANES)) for i in range(STRIP)
    ]
    for i in range(STRIP):
        inverse = lax.rsqrt(columns[i][i : i + 1, :])
        scaled = columns[i] * inverse
        for k in range(i + 1, STRIP):
            base = k // SUBLANES * SUBLANES
            low = columns[k][base:] - scaled[base:] * scaled[k : k + 1, :]
            columns[k] = low if base == 0 else jnp.concatenate([columns[k][:base], low], axis=0)
        factor = jnp.where(row > i, scaled, 0.0)
        for v, x in enumerate(values):
            pivot = x[i : i + 1, :] * inverse
            values[v] = jnp.where(row == i, pivot, x - factor * pivot)
    for (ref, at, _), x in zip(parts, values):
        if ref is r_ref:
            x = jnp.where(col + at >= row + start, x, 0.0)
        else:
            x = jnp.where(col + at <= row + start, x, 0.0)
        ref[rows, at : at + LANES] = x


class Direct:
    def __init__(self, members, member, device, size, source, landing, result, base, sems):
        self.members, self.member, self.device = members, member, device
        self.source, self.landing, self.result, self.base, self.sems = source, landing, result, base, sems
        self.owners = min(members, size // SUBLANES)
        self.piece = size // self.owners

    def rows(self, index, base=0):
        return pl.ds(pl.multiple_of(base + index * self.piece, SUBLANES), self.piece)

    def if_owner(self, index, body):
        if self.owners == self.members:
            body()
        else:
            pl.when(index < self.owners)(body)

    def each(self, body):
        def step(k, carry):
            body(lax.rem(self.member + k, self.members))
            return carry

        lax.fori_loop(1, self.members, step, 0, unroll=self.members <= 4)

    def wait(self, ref, sem):
        pltpu.make_async_copy(ref, ref, sem).wait()

    def wait_parts(self, sem):
        def whole(parts):
            self.wait(self.result.at[pl.ds(0, parts * self.piece)], sem)

        if self.owners == self.members:
            whole(self.owners - 1)
        else:
            pl.when(self.member < self.owners)(lambda: whole(self.owners - 1))
            pl.when(self.member >= self.owners)(lambda: whole(self.owners))

    def scatter(self):
        def send(target):
            self.if_owner(target, lambda: pltpu.make_async_remote_copy(
                src_ref=self.source.at[self.rows(target)], dst_ref=self.landing.at[self.member],
                send_sem=self.sems.at[0], recv_sem=self.sems.at[1],
                device_id=self.device(target), device_id_type=MESH,
            ).start())

        self.each(send)

    def reduce(self):
        @functools.partial(self.if_owner, self.member)
        def _():
            index = lax.rem(self.member, self.owners)
            mine = self.rows(index, self.base)
            self.landing[self.member] = self.source[self.rows(index), :]
            self.wait(self.landing.at[pl.ds(0, self.members - 1)], self.sems.at[1])
            self.result[mine, :] = jnp.sum(self.landing[...], axis=0)
            self.each(lambda target: pltpu.make_async_remote_copy(
                src_ref=self.result.at[mine], dst_ref=self.result.at[mine],
                send_sem=self.sems.at[2], recv_sem=self.sems.at[3],
                device_id=self.device(target), device_id_type=MESH,
            ).start())

    def arrived(self):
        self.wait_parts(self.sems.at[3])

    def finish(self):
        self.wait_parts(self.sems.at[0])
        self.if_owner(self.member, lambda: self.wait(
            self.landing.at[pl.ds(0, self.members - 1)], self.sems.at[2]))


class Pair:
    def __init__(self, side, device, half, source, base, landing, kept, sems):
        self.device, self.source, self.landing, self.kept, self.sems = device, source, landing, kept, sems
        self.mine = pl.ds(pl.multiple_of(base + side * half, SUBLANES), half)
        self.other = pl.ds(pl.multiple_of(base + (1 - side) * half, SUBLANES), half)

    def scatter(self):
        self.out = pltpu.make_async_remote_copy(
            src_ref=self.source.at[self.other], dst_ref=self.landing,
            send_sem=self.sems.at[0], recv_sem=self.sems.at[1],
            device_id=self.device, device_id_type=MESH,
        )
        self.out.start()

    def reduce(self):
        self.out.wait_recv()
        self.kept[...] = self.source[self.mine, :] + self.landing[...]

    def gather(self, result):
        self.back = pltpu.make_async_remote_copy(
            src_ref=result.at[self.mine], dst_ref=result.at[self.mine],
            send_sem=self.sems.at[2], recv_sem=self.sems.at[3],
            device_id=self.device, device_id_type=MESH,
        )
        self.back.start()

    def arrived(self):
        self.back.wait_recv()

    def finish(self):
        self.out.wait_send()
        self.back.wait_send()


def gather_and_factor(
    nrows, ncols, panel_ref, trailing_ref, r_ref, y_ref, cross_ref, block_ref,
    held, high, low, pieces, gram, gram_near, gram_pair, gram_in, gram_sum,
    share, share_near, share_pair, share_in, total,
    load_sem, piece_send, piece_recv, gram_pair_sem, gram_sem, share_pair_sem, share_sem,
):
    r, c = lax.axis_index("rows"), lax.axis_index("cols")
    depth, n = panel_ref.shape
    chunks = n // CHUNK

    own_load = pltpu.make_async_copy(panel_ref, pieces.at[c], load_sem.at[0])
    own_load.start()
    load = pltpu.make_async_copy(trailing_ref, held, load_sem.at[1])
    load.start()
    own_load.wait()

    bits = [1 << b for b in reversed(range(ncols.bit_length() - 1))]
    sent = []

    def pass_on(offset, bit, chunk):
        slot = jnp.bitwise_xor(c, offset)
        view = pieces.at[slot, :, pl.ds(chunk * CHUNK, CHUNK)]
        copy = pltpu.make_async_remote_copy(
            src_ref=view, dst_ref=view,
            send_sem=piece_send.at[len(sent)], recv_sem=piece_recv.at[len(sent)],
            device_id=(r, jnp.bitwise_xor(c, bit)), device_id_type=MESH,
        )
        copy.start()
        sent.append(copy)
        return offset ^ bit, copy

    coming = {(bit, chunk): [pass_on(0, bit, chunk)] for chunk in range(chunks) for bit in bits}

    gram[...] = contract(pieces[c], pieces[c], ((0,), (0,)))
    side, wide = lax.rem(c, 2), ncols // 2
    gram_halves = Pair(side, (r, jnp.bitwise_xor(c, 1)), n // 2, gram, 0, gram_near, gram_pair, gram_pair_sem)
    gram_halves.scatter()
    gram_all = Direct(
        nrows * wide, r * wide + lax.div(c, 2),
        lambda t: (lax.div(t, wide), lax.rem(t, wide) * 2 + side),
        n // 2, gram_pair, gram_in, gram_sum, side * (n // 2), gram_sem,
    )
    upper = lax.rem(r, 2)
    pairs, groups = [], []
    for h in range(chunks):
        half = CHUNK // 2
        pairs.append(Pair(
            upper, (jnp.bitwise_xor(r, 1), c), half, share, h * CHUNK,
            share_near.at[h], share_pair.at[h], share_pair_sem.at[h],
        ))
        groups.append(Direct(
            nrows // 2, lax.div(r, 2), lambda t: (t * 2 + upper, c),
            half, share_pair.at[h], share_in.at[h], total, h * CHUNK + upper * half, share_sem.at[h],
        ))

    load.wait()

    def split(i, carry):
        at = pl.ds(pl.multiple_of(i * LANES, LANES), LANES)
        high[at, :], low[at, :] = halves(held[at, :])
        return carry

    lax.fori_loop(0, held.shape[0] // LANES, split, 0)
    gram_halves.reduce()
    gram_all.scatter()

    def multiply(offset, h, first=False):
        slot = jnp.bitwise_xor(c, offset)
        at = pl.ds(pl.multiple_of(slot * depth, LANES), depth)
        mine = slice(h * CHUNK, (h + 1) * CHUNK)
        product = contract3(halves(pieces[slot, :, mine]), (high[at, :], low[at, :]), ((0,), (0,)))
        share[mine, :] = product if first else share[mine, :] + product

    for h in range(chunks):
        multiply(0, h, True)
    for h in range(chunks):
        offset, copy = coming[bits[-1], h].pop(0)
        copy.wait_recv()
        multiply(offset, h)

    def take(h):
        for at, bit in enumerate(bits):
            for offset, copy in coming[bit, h]:
                copy.wait_recv()
                for later in bits[at + 1 :]:
                    coming[later, h].append(pass_on(offset, later, h))
                multiply(offset, h)
        pairs[h].scatter()

    strips = list(range(0, n, STRIP))

    def factor(some):
        for start in some:
            if start >= LANES:
                r_ref[start : start + STRIP, 0 : start // LANES * LANES] = jnp.zeros(
                    (STRIP, start // LANES * LANES), F32
                )
            edge = -(-(start + STRIP) // LANES) * LANES
            if edge < n:
                y_ref[start : start + STRIP, edge:n] = jnp.zeros((STRIP, n - edge), F32)
            factor_strip(start, gram_sum, r_ref, y_ref)

    take(0)
    gram_all.reduce()
    for h in range(1, chunks):
        pairs[h - 1].reduce()
        groups[h - 1].scatter()
        take(h)
        groups[h - 1].reduce()
    block_out = pltpu.make_async_copy(pieces, block_ref, load_sem.at[1])
    block_out.start()
    gram_all.arrived()
    gram_halves.gather(gram_sum)
    pairs[-1].reduce()
    groups[-1].scatter()
    gram_halves.arrived()
    half = len(strips) // 2
    factor(strips[:half])
    groups[-1].reduce()
    for h in range(chunks - 1):
        groups[h].arrived()
        pairs[h].gather(total)
    factor(strips[half:])
    groups[-1].arrived()
    pairs[-1].gather(total)
    for pair in pairs:
        pair.arrived()
    cross_ref[...] = total[...]
    for copy in sent:
        copy.wait_send()
    for exchange in [gram_halves, gram_all] + pairs + groups:
        exchange.finish()
    block_out.wait()


def update(r_ref, y_ref, cross_ref, block_ref, trailing_ref, r_out, projected_ref, updated_ref, high, low):
    @pl.when(pl.program_id(0) == 0)
    def _():
        r_out[...] = r_ref[...]
        projected = contract(y_ref[...], cross_ref[...], ((1,), (0,)))
        projected_ref[...] = projected
        high[...], low[...] = halves(contract(y_ref[...], projected, ((0,), (0,))))

    product = contract3(halves(block_ref[...]), (high[...], low[...]), ((1,), (0,)))
    updated_ref[...] = trailing_ref[...] - product


def solution(mesh):
    nrows, ncols = mesh.shape["rows"], mesh.shape["cols"]

    def shards(panel, trailing):
        depth, n = panel.shape
        height, width = trailing.shape
        chunks = n // CHUNK
        half = CHUNK // 2
        group = nrows * ncols // 2
        vmem = pl.BlockSpec(memory_space=pltpu.VMEM)
        hbm = pl.BlockSpec(memory_space=pl.ANY)
        r, y, cross, block = pl.pallas_call(
            functools.partial(gather_and_factor, nrows, ncols),
            name="gather_and_factor",
            out_shape=(
                jax.ShapeDtypeStruct((n, n), F32),
                jax.ShapeDtypeStruct((n, n), F32),
                jax.ShapeDtypeStruct((n, width), F32),
                jax.ShapeDtypeStruct((ncols, depth, n), F32),
            ),
            in_specs=[hbm, hbm],
            out_specs=(vmem, vmem, vmem, hbm),
            scratch_shapes=[
                pltpu.VMEM((height, width), F32),
                pltpu.VMEM((height, width), jnp.bfloat16),
                pltpu.VMEM((height, width), jnp.bfloat16),
                pltpu.VMEM((ncols, depth, n), F32),
                pltpu.VMEM((n, n), F32),
                pltpu.VMEM((n // 2, n), F32),
                pltpu.VMEM((n // 2, n), F32),
                pltpu.VMEM((group, n // 2 // min(group, n // 2 // SUBLANES), n), F32),
                pltpu.VMEM((n, n), F32),
                pltpu.VMEM((n, width), F32),
                pltpu.VMEM((chunks, half, width), F32),
                pltpu.VMEM((chunks, half, width), F32),
                pltpu.VMEM((chunks, nrows // 2, half // min(nrows // 2, half // SUBLANES), width), F32),
                pltpu.VMEM((n, width), F32),
                pltpu.SemaphoreType.DMA((2,)),
                pltpu.SemaphoreType.DMA(((ncols - 1) * chunks,)),
                pltpu.SemaphoreType.DMA(((ncols - 1) * chunks,)),
                pltpu.SemaphoreType.DMA((4,)),
                pltpu.SemaphoreType.DMA((4,)),
                pltpu.SemaphoreType.DMA((chunks, 4)),
                pltpu.SemaphoreType.DMA((chunks, 4)),
            ],
            compiler_params=pltpu.CompilerParams(has_side_effects=True, vmem_limit_bytes=67043328),
        )(panel, trailing)
        block = block.reshape(height, n)
        tile = min(height, 256)
        whole = lambda *shape: pl.BlockSpec(shape, lambda i: (0, 0))
        tall = lambda wide: pl.BlockSpec((tile, wide), lambda i: (i, 0))
        return pl.pallas_call(
            update,
            name="update",
            grid=(height // tile,),
            out_shape=(
                jax.ShapeDtypeStruct((n, n), F32),
                jax.ShapeDtypeStruct((n, width), F32),
                jax.ShapeDtypeStruct((height, width), F32),
            ),
            in_specs=[whole(n, n), whole(n, n), whole(n, width), tall(n), tall(width)],
            out_specs=(whole(n, n), whole(n, width), tall(width)),
            scratch_shapes=[pltpu.VMEM((n, width), jnp.bfloat16)] * 2,
            compiler_params=pltpu.CompilerParams(vmem_limit_bytes=67043328),
        )(r, y, cross, block, trailing)

    placed = (P(("rows", "cols"), None), P("rows", "cols"))
    return jax.shard_map(
        shards,
        mesh=mesh,
        in_specs=placed,
        out_specs=(P(), P(None, "cols"), P("rows", "cols")),
        check_vma=False,
    )
```
